32 devices in a mesh: dp: 1 (over z), row: 4 (over y), col: 8 (over x, core).
Axes of the slice: x: 4, y: 4, z: 1, core: 2. Of those that a mesh axis runs over, the one named last changes fastest.
The devices are a block of a 4x4x8 slice.
Arguments:
- x: bfloat16 [2, 32, 512, 2048], P(None, ('dp', 'row', 'col'))
- idx: int32 [2, 32, 512, 8], P(None, ('dp', 'row', 'col'))
- gates: float32 [2, 32, 512, 8], P(None, ('dp', 'row', 'col'))
- wq: bfloat16 [2048, 4096], replicated
- wk: bfloat16 [2048, 4096], replicated
- wv: bfloat16 [2048, 4096], replicated
- wo: bfloat16 [4096, 2048], replicated
- gattn: float32 [2048], replicated
- gmoe: float32 [2048], replicated
- w1: bfloat16 [128, 2048, 768], P(('row', 'col'))
- w3: bfloat16 [128, 2048, 768], P(('row', 'col'))
- w2: bfloat16 [128, 768, 2048], P(('row', 'col'))
Outputs:
- output: bfloat16 [2, 32, 512, 2048], P(None, ('dp', 'row', 'col'))
All inputs are finite; a program needn't handle non-finite values.
Results may differ from the reference program's by a relative error of at most 0.00847974.
Values are sent between devices in bfloat16 or wider.
A program may use at most 768 MiB of HBM per device.

```python
import jax
import jax.numpy as jnp
from jax import lax

D = 2048
HEADS = 32
HEAD = 128
EXPERTS = 128
TOP = 8
FF = 768
TOKENS = 512
SEQ = 512
GROUP = 32

CAP = ((TOP * ((2 * TOKENS + EXPERTS - 1) // EXPERTS) + 7) // 8) * 8
NTOK = GROUP * TOKENS
NSEQ = NTOK // SEQ


def draw_routing(key):
    k1, k2, k3 = jax.random.split(key, 3)
    k1 = jax.random.fold_in(k1, 7919)
    k2 = jax.random.fold_in(k2, 7919)
    offset = jax.random.randint(k1, (), 0, EXPERTS)
    ranks = jax.vmap(lambda kk: jax.random.permutation(kk, TOKENS))(jax.random.split(k2, GROUP))
    half = TOKENS // 2
    quarter = EXPERTS // 4
    r = jnp.where(ranks < half, (ranks * quarter) // half, quarter + ((ranks - half) * (EXPERTS - quarter)) // half)
    pos = (offset + r[:, :, None] - jnp.arange(TOP)[None, None, :]) % EXPERTS
    idx = pos.reshape(NSEQ, SEQ, TOP).astype(jnp.int32)
    gates = jax.nn.softmax(jax.random.normal(k3, (NSEQ, SEQ, TOP), jnp.float32), axis=-1)
    return idx, gates


def setup_inputs(seed: int = 0, part: int = 0) -> dict:
    key = jax.random.key(seed)
    kw = jax.random.split(key, 10)
    kp = jax.random.split(jax.random.fold_in(key, part), 4)
    hd = HEADS * HEAD
    base = jax.random.normal(kp[0], (2, NSEQ, SEQ, D), jnp.float32)
    shift = 0.8 * jax.random.normal(kp[1], (2, NSEQ, 1, D), jnp.float32)
    x = (base + shift).astype(jnp.bfloat16)
    ia, ga = draw_routing(kp[2])
    ib, gb = draw_routing(kp[3])
    idx = jnp.stack([ia, ib])
    gates = jnp.stack([ga, gb])
    wq = (jax.random.normal(kw[0], (D, hd), jnp.float32) * D ** -0.5).astype(jnp.bfloat16)
    wk = (jax.random.normal(kw[1], (D, hd), jnp.float32) * D ** -0.5).astype(jnp.bfloat16)
    wv = (jax.random.normal(kw[2], (D, hd), jnp.float32) * D ** -0.5).astype(jnp.bfloat16)
    wo = (jax.random.normal(kw[3], (hd, D), jnp.float32) * hd ** -0.5).astype(jnp.bfloat16)
    gattn = 1.0 + 0.3 * jax.random.normal(kw[4], (D,), jnp.float32)
    gmoe = 1.0 + 0.3 * jax.random.normal(kw[5], (D,), jnp.float32)
    w1 = (jax.random.normal(kw[6], (EXPERTS, D, FF), jnp.float32) * D ** -0.5).astype(jnp.bfloat16)
    w3 = (jax.random.normal(kw[7], (EXPERTS, D, FF), jnp.float32) * D ** -0.5).astype(jnp.bfloat16)
    w2 = (jax.random.normal(kw[8], (EXPERTS, FF, D), jnp.float32) * 2.0 * FF ** -0.5).astype(jnp.bfloat16)
    return {"x": x, "idx": idx, "gates": gates, "wq": wq, "wk": wk, "wv": wv, "wo": wo, "gattn": gattn, "gmoe": gmoe, "w1": w1, "w3": w3, "w2": w2}


def rms(v, g):
    vf = v.astype(jnp.float32)
    return (vf * lax.rsqrt(jnp.mean(vf * vf, axis=-1, keepdims=True) + 1e-6) * g).astype(jnp.bfloat16)


def attention(x, wq, wk, wv, wo, gattn):
    u = rms(x, gattn)

    def proj(w):
        a = jnp.dot(u, w, preferred_element_type=jnp.float32).astype(jnp.bfloat16)
        return a.reshape(NSEQ, SEQ, HEADS, HEAD).transpose(2, 0, 1, 3)

    q, k, v = proj(wq), proj(wk), proj(wv)
    causal = jnp.arange(SEQ)[:, None] >= jnp.arange(SEQ)[None, :]

    def one_head(qkv):
        qh, kh, vh = qkv
        s = jnp.einsum("cre,cle->crl", qh.astype(jnp.float32), kh.astype(jnp.float32)) * HEAD ** -0.5
        s = jnp.where(causal[None], s, -1e30)
        p = jax.nn.softmax(s, axis=-1).astype(jnp.bfloat16)
        o = jnp.einsum("crl,cle->cre", p.astype(jnp.float32), vh.astype(jnp.float32))
        return o.astype(jnp.bfloat16)

    o = lax.map(one_head, (q, k, v))
    o = o.transpose(1, 2, 0, 3).reshape(NTOK, HEADS * HEAD)
    a = jnp.dot(o, wo, preferred_element_type=jnp.float32)
    return (x.astype(jnp.float32) + a).astype(jnp.bfloat16)


def moe(h, idx, gates, w1, w3, w2, gmoe):
    z = rms(h, gmoe)
    zpad = jnp.concatenate([z, jnp.zeros((1, D), jnp.bfloat16)], axis=0)
    flat = idx.reshape(-1)
    gflat = gates.reshape(-1)
    order = jnp.argsort(flat, stable=True)
    counts = jnp.zeros((EXPERTS,), jnp.int32).at[flat].add(1)
    starts = jnp.cumsum(counts) - counts
    width = GROUP * CAP

    def step(acc, per_expert):
        a1, a3, a2, st, ct = per_expert
        slot = st + jnp.arange(width)
        valid = slot < st + ct
        pair = order[jnp.minimum(slot, NTOK * TOP - 1)]
        tok = jnp.where(valid, pair // TOP, NTOK)
        gate = jnp.where(valid, gflat[pair], 0.0)
        rows = zpad[tok]
        h1 = jnp.dot(rows, a1, preferred_element_type=jnp.float32)
        h3 = jnp.dot(rows, a3, preferred_element_type=jnp.float32)
        act = (jax.nn.silu(h1) * h3).astype(jnp.bfloat16)
        out = jnp.dot(act, a2, preferred_element_type=jnp.float32).astype(jnp.bfloat16)
        acc = acc.at[tok].add(gate[:, None] * out.astype(jnp.float32), mode="drop")
        return acc, None

    acc, _ = lax.scan(step, jnp.zeros((NTOK, D), jnp.float32), (w1, w3, w2, starts, counts))
    return (h.astype(jnp.float32) + acc).astype(jnp.bfloat16)


def reference(x, idx, gates, wq, wk, wv, wo, gattn, gmoe, w1, w3, w2):
    ys = []
    for m in range(2):
        h = attention(x[m].reshape(NTOK, D), wq, wk, wv, wo, gattn)
        y = moe(h, idx[m].reshape(NTOK, TOP), gates[m].reshape(NTOK, TOP), w1, w3, w2, gmoe)
        ys.append(y.reshape(NSEQ, SEQ, D))
    return jnp.stack(ys)
```

```python
import functools

import jax
import jax.numpy as jnp
from jax import lax
from jax.experimental import pallas as pl
from jax.experimental.pallas import tpu as pltpu
from jax.sharding import PartitionSpec as P

HEAD = 128
VMEM_LIMIT = 67_000_000
CORES = 2
SLOTS = 128


def capacity(t, top, n_exp):
    return ((top * ((2 * t + n_exp - 1) // n_exp) + 7) // 8) * 8


def rms(vf, g):
    return (vf * lax.rsqrt(jnp.mean(vf * vf, axis=-1, keepdims=True) + 1e-6) * g).astype(jnp.bfloat16)


def pieces(v):
    out = []
    for _ in range(3):
        p = v.astype(jnp.bfloat16)
        out.append(p)
        v = v - p.astype(jnp.float32)
    return out


def dot(a, b, dims=((1,), (0,))):
    return lax.dot_general(a, b, (dims, ((), ())), preferred_element_type=jnp.float32)


def attention_body(nh, x_ref, ga_ref, gm_ref, wq_ref, wk_ref, wv_ref, wo_ref, h_ref, z_ref, u_ref, acc_ref):
    i = pl.program_id(0)

    @pl.when(i == 0)
    def _():
        u_ref[...] = rms(x_ref[...].astype(jnp.float32), ga_ref[...])
        acc_ref[...] = jnp.zeros_like(acc_ref)

    u = u_ref[...]
    seq = u.shape[0]
    half = seq // 2
    q = dot(u, wq_ref[...]).astype(jnp.bfloat16)
    k = dot(u, wk_ref[...]).astype(jnp.bfloat16)
    v = dot(u, wv_ref[...]).astype(jnp.bfloat16)
    tops, lows = [], []
    for j in range(nh):
        cols = slice(j * HEAD, (j + 1) * HEAD)
        for part, dst in ((0, tops), (1, lows)):
            n = half * (part + 1)
            s = dot(q[part * half:(part + 1) * half, cols], k[:n, cols], ((1,), (1,))) * HEAD ** -0.5
            row = lax.broadcasted_iota(jnp.int32, s.shape, 0) + part * half
            col = lax.broadcasted_iota(jnp.int32, s.shape, 1)
            s = jnp.where(row >= col, s, -1e30)
            e = jnp.exp(s - jnp.max(s, axis=-1, keepdims=True))
            p = (e * (1.0 / jnp.sum(e, axis=-1, keepdims=True))).astype(jnp.bfloat16)
            dst.append(dot(p, v[:n, cols]).astype(jnp.bfloat16))
    o = jnp.concatenate([jnp.concatenate(tops, axis=1), jnp.concatenate(lows, axis=1)], axis=0)
    acc_ref[...] += dot(o, wo_ref[...])

    @pl.when(i == pl.num_programs(0) - 1)
    def _():
        h = (x_ref[...].astype(jnp.float32) + acc_ref[...]).astype(jnp.bfloat16)
        h_ref[...] = h
        z_ref[...] = rms(h.astype(jnp.float32), gm_ref[...])


def attention(x, gattn, gmoe, wq, wk, wv, wo):
    seq, d = x.shape
    hd = wq.shape[1]
    nh = 2
    blk = nh * HEAD
    whole = lambda r: pl.BlockSpec((r, d), lambda i: (0, 0))
    wcol = pl.BlockSpec((d, blk), lambda i: (0, i))
    act = jax.ShapeDtypeStruct((seq, d), jnp.bfloat16)
    flops = 2 * seq * d * hd * 4 + 4 * seq * seq * hd
    return pl.pallas_call(
        functools.partial(attention_body, nh),
        grid=(hd // blk,),
        in_specs=[whole(seq), whole(1), whole(1), wcol, wcol, wcol, pl.BlockSpec((blk, d), lambda i: (i, 0))],
        out_specs=[whole(seq), whole(seq)],
        out_shape=[act, act],
        scratch_shapes=[pltpu.VMEM((seq, d), jnp.bfloat16), pltpu.VMEM((seq, d), jnp.float32)],
        compiler_params=pltpu.CompilerParams(vmem_limit_bytes=VMEM_LIMIT),
        cost_estimate=pl.CostEstimate(flops=flops, bytes_accessed=8 * d * hd, transcendentals=seq * seq * hd // HEAD),
        name="attn",
    )(x, gattn.reshape(1, d), gmoe.reshape(1, d), wq, wk, wv, wo)


def dispatch_body(slot_ref, z_ref, o_ref):
    slot = slot_ref[0]
    k = lax.broadcasted_iota(jnp.int32, (o_ref.shape[1], slot.shape[1]), 0)
    o_ref[0] = dot((slot == k).astype(jnp.bfloat16), z_ref[...]).astype(jnp.bfloat16)


def dispatch(slot, z):
    nc, _, t = slot.shape
    d = z.shape[1]
    return pl.pallas_call(
        dispatch_body,
        grid=(nc,),
        in_specs=[pl.BlockSpec((1, 1, t), lambda i: (i, 0, 0)), pl.BlockSpec((t, d), lambda i: (0, 0))],
        out_specs=pl.BlockSpec((1, SLOTS, d), lambda i: (i, 0, 0)),
        out_shape=jax.ShapeDtypeStruct((nc, SLOTS, d), jnp.bfloat16),
        compiler_params=pltpu.CompilerParams(vmem_limit_bytes=VMEM_LIMIT),
        cost_estimate=pl.CostEstimate(flops=2 * nc * SLOTS * t * d, bytes_accessed=2 * nc * SLOTS * d, transcendentals=0),
        name="dispatch",
    )(slot, z)


def experts_body(ns, cap, own_ref, oth_ref, pos_ref, g_ref, w1_hbm, w3_hbm, w2_hbm, pown_ref, poth_ref,
                 w1_ref, w3_ref, w2_ref, x_ref, o_ref, sems):
    i = pl.program_id(0)
    el = w1_ref.shape[0]

    def loads(e):
        return [pltpu.make_async_copy(src.at[e], dst.at[e], sems.at[j, e])
                for j, (src, dst) in enumerate(((w1_hbm, w1_ref), (w3_hbm, w3_ref), (w2_hbm, w2_ref)))]

    @pl.when(i == 0)
    def _():
        for e in range(el):
            for c in loads(e):
                c.start()

    slots = pos_ref.shape[2]
    rank = lax.broadcasted_iota(jnp.int32, (el, cap, slots), 1)
    for s in range(ns):
        rows = jnp.concatenate([own_ref[s], oth_ref[s]], axis=0)
        hit = (pos_ref[s][:, None, :] == rank).astype(jnp.bfloat16).reshape(el * cap, slots)
        xs = dot(hit, rows).astype(jnp.bfloat16)
        for e in range(el):
            x_ref[e, s * cap:(s + 1) * cap, :] = xs[e * cap:(e + 1) * cap]

    def expert(e, _):
        @pl.when(i == 0)
        def _():
            for c in loads(e):
                c.wait()

        x = x_ref[e]
        h1 = dot(x, w1_ref[e])
        h3 = dot(x, w3_ref[e])
        a = (jax.nn.silu(h1) * h3).astype(jnp.bfloat16)
        o = dot(a, w2_ref[e]).astype(jnp.bfloat16)
        for s in range(ns):
            o_ref[s, e] = o[s * cap:(s + 1) * cap]
        return 0

    lax.fori_loop(0, el, expert, 0)

    for s in range(ns):
        w = jnp.where(pos_ref[s][:, None, :] == rank, g_ref[s][:, None, :], 0.0).reshape(el * cap, slots)
        w = jnp.concatenate(pieces(w), axis=1)
        p3 = dot(w, o_ref[s].reshape(el * cap, -1), ((0,), (0,)))
        p = p3[:slots] + p3[slots:2 * slots] + p3[2 * slots:]
        pown_ref[s] = p[:slots // CORES]
        poth_ref[s] = p[slots // CORES:]


def experts(own, oth, pos, g, w1, w3, w2, cap):
    n, half, d = own.shape
    el, _, f = w1.shape
    ns = 4
    slots = pos.shape[2]
    rows = pl.BlockSpec((ns, half, d), lambda i: (i, 0, 0))
    meta = pl.BlockSpec((ns, el, slots), lambda i: (i, 0, 0))
    hbm = pl.BlockSpec(memory_space=pl.ANY)
    part = jax.ShapeDtypeStruct((n, half, d), jnp.float32)
    flops = 6 * n * el * cap * d * f
    return pl.pallas_call(
        functools.partial(experts_body, ns, cap),
        grid=(n // ns,),
        in_specs=[rows, rows, meta, meta, hbm, hbm, hbm],
        out_specs=[rows, rows],
        out_shape=[part, part],
        scratch_shapes=[
            pltpu.VMEM((el, d, f), jnp.bfloat16),
            pltpu.VMEM((el, d, f), jnp.bfloat16),
            pltpu.VMEM((el, f, d), jnp.bfloat16),
            pltpu.VMEM((el, ns * cap, d), jnp.bfloat16),
            pltpu.VMEM((ns, el, cap, d), jnp.bfloat16),
            pltpu.SemaphoreType.DMA((3, el)),
        ],
        compiler_params=pltpu.CompilerParams(vmem_limit_bytes=VMEM_LIMIT),
        cost_estimate=pl.CostEstimate(flops=flops, bytes_accessed=6 * el * d * f + 12 * n * half * d, transcendentals=n * el * cap * f),
        name="experts",
    )(own, oth, pos, g, w1, w3, w2)


def combine_body(slot_ref, ret_ref, h_ref, acc_in_ref, y_ref, acc_ref):
    i = pl.program_id(0)

    @pl.when(i == 0)
    def _():
        acc_ref[...] = acc_in_ref[...] if acc_in_ref is not None else jnp.zeros_like(acc_ref)

    nc, slots, d = ret_ref.shape
    t = slot_ref.shape[2]
    k = lax.broadcasted_iota(jnp.int32, (slots, t), 0)
    sel = jnp.concatenate([(slot_ref[c] == k).astype(jnp.bfloat16) for c in range(nc)], axis=0)
    for p in pieces(ret_ref[...].reshape(nc * slots, d)):
        acc_ref[...] += dot(sel, p, ((0,), (0,)))

    @pl.when(i == pl.num_programs(0) - 1)
    def _():
        y_ref[...] = (h_ref[...].astype(jnp.float32) + acc_ref[...]).astype(jnp.bfloat16)


def combine(slot, ret, h, acc=None):
    nc, _, t = slot.shape
    d = h.shape[1]
    nb = 2
    whole = pl.BlockSpec((t, d), lambda i: (0, 0))
    specs = [pl.BlockSpec((nb, 1, t), lambda i: (i, 0, 0)), pl.BlockSpec((nb, SLOTS, d), lambda i: (i, 0, 0)), whole]
    args = [slot, ret, h]
    body = combine_body
    if acc is None:
        body = lambda s, r, h, y, a: combine_body(s, r, h, None, y, a)
    else:
        specs.append(whole)
        args.append(acc)
    return pl.pallas_call(
        body,
        grid=(nc // nb,),
        in_specs=specs,
        out_specs=[whole, whole],
        out_shape=[jax.ShapeDtypeStruct((t, d), jnp.bfloat16), jax.ShapeDtypeStruct((t, d), jnp.float32)],
        compiler_params=pltpu.CompilerParams(vmem_limit_bytes=VMEM_LIMIT),
        cost_estimate=pl.CostEstimate(flops=6 * nc * SLOTS * t * d, bytes_accessed=4 * nc * SLOTS * d, transcendentals=0),
        name="combine",
    )(*args)


def chip_ranks(idx, nc, epc):
    t = idx.shape[0]
    hit = jnp.any((idx // epc)[:, :, None] == jnp.arange(nc, dtype=idx.dtype), axis=1)
    tri = (jnp.arange(t)[:, None] > jnp.arange(t)[None, :]).astype(jnp.bfloat16)
    rank = dot(tri, hit.astype(jnp.bfloat16)).astype(jnp.int32)
    return jnp.where(hit, rank, -1).T.reshape(nc, 1, t), jnp.max(jnp.sum(hit, axis=0))


def slot_gates(slot, gm):
    nc, _, t = slot.shape
    sel = (slot == jnp.arange(SLOTS, dtype=jnp.int32)[None, :, None]).astype(jnp.bfloat16)
    g = jnp.stack(pieces(gm.reshape(t, nc, -1)))
    out = jnp.einsum("ckt,ptce->pcek", sel, g, preferred_element_type=jnp.float32)
    return out[0] + (out[1] + out[2])


def solution(mesh):
    ep_axes = ("row", "col")
    tok_axes = ("dp", "row", "col")
    ncol = mesh.shape["col"]
    ep = mesh.shape["row"] * ncol
    nc = ep // CORES
    pair = [(i, i ^ 1) for i in range(ncol)]

    def local(x, idx, gates, wq, wk, wv, wo, gattn, gmoe, w1, w3, w2):
        nm, ns, seq, d = x.shape
        t = ns * seq
        top = idx.shape[-1]
        el = w1.shape[0]
        n_exp = el * ep
        cap = capacity(t, top, n_exp)
        odd = lax.axis_index("col") % CORES == 1

        ranks, most, dense = [], [], []
        for m in range(nm):
            im = idx[m].reshape(t, top)
            rank, count = chip_ranks(im, nc, n_exp // nc)
            ranks.append(rank)
            most.append(count)
            hit = im[:, :, None] == jnp.arange(n_exp, dtype=im.dtype)
            dense.append(jnp.sum(jnp.where(hit, gates[m].reshape(t, top)[:, :, None], 0.0), axis=1))

        def exchange_gates(r):
            g = [slot_gates(ranks[m] - r * SLOTS, dense[m]).reshape(ep, el, SLOTS) for m in range(nm)]
            top_count = functools.reduce(jnp.maximum, most).astype(jnp.float32)
            g.append(jnp.broadcast_to(top_count, (ep, 8, SLOTS)))
            got = lax.all_to_all(jnp.concatenate(g, axis=1), ep_axes, 0, 0, tiled=True)
            out = []
            for m in range(nm):
                gm = got[:, m * el:(m + 1) * el]
                gm = jnp.where(odd, jnp.roll(gm, SLOTS // CORES, axis=-1), gm)
                hit = gm > 0.0
                tri = (jnp.arange(SLOTS)[:, None] < jnp.arange(SLOTS)[None, :]).astype(jnp.bfloat16)
                pos = dot(hit.astype(jnp.bfloat16).reshape(ep * el, SLOTS), tri).astype(jnp.int32).reshape(hit.shape)
                out.append((jnp.where(hit, pos, -1), gm))
            return out, jnp.max(got[:, nm * el:])

        def send(m, r, z):
            slot = ranks[m] - r * SLOTS
            buf = dispatch(slot, z).reshape(ep, SLOTS // CORES, d)
            own = lax.all_to_all(buf, ep_axes, 0, 0, tiled=True)
            return own, lax.ppermute(own, "col", pair)

        def give_back(own, oth, meta):
            pown, poth = experts(own, oth, meta[0], meta[1], w1, w3, w2, cap)
            total = pown + lax.ppermute(poth, "col", pair)
            return lax.all_to_all(total, ep_axes, 0, 0, tiled=True).reshape(nc, SLOTS, d)

        meta, most_all = exchange_gates(0)
        hs, zs = [], []
        recv = []
        for m in range(nm):
            h, z = attention(x[m].reshape(t, d), gattn, gmoe, wq, wk, wv, wo)
            hs.append(h)
            zs.append(z)
            recv.append(send(m, 0, z))
        ys, accs = [], []
        for m in range(nm):
            ret = give_back(*recv[m], meta[m])
            y, acc = combine(ranks[m], ret, hs[m])
            ys.append(y)
            accs.append(acc)

        rounds = (most_all.astype(jnp.int32) + SLOTS - 1) // SLOTS

        def more(c):
            r, ys, accs = c
            meta, _ = exchange_gates(r)
            ny, na = [], []
            for m in range(nm):
                ret = give_back(*send(m, r, zs[m]), meta[m])
                y, acc = combine(ranks[m] - r * SLOTS, ret, hs[m], accs[m])
                ny.append(y)
                na.append(acc)
            return r + 1, tuple(ny), tuple(na)

        _, ys, _ = lax.while_loop(lambda c: c[0] < rounds, more, (jnp.int32(1), tuple(ys), tuple(accs)))
        return jnp.stack([y.reshape(ns, seq, d) for y in ys])

    tok_spec = P(None, tok_axes)
    exp_spec = P(ep_axes)
    return jax.shard_map(local, mesh=mesh,
                         in_specs=(tok_spec, tok_spec, tok_spec, P(), P(), P(), P(), P(), P(), exp_spec, exp_spec, exp_spec),
                         out_specs=tok_spec, check_vma=False)
```

```python
import functools

import jax
import jax.numpy as jnp
from jax import lax
from jax.experimental import pallas as pl
from jax.experimental.pallas import tpu as pltpu
from jax.sharding import PartitionSpec as P


HEAD = 128
VMEM_LIMIT = 67_000_000
CORES = 2
SLOTS = 128


def capacity(t, top, n_exp):
    return ((top * ((2 * t + n_exp - 1) // n_exp) + 7) // 8) * 8


def rms(vf, g):
    return (vf * lax.rsqrt(jnp.mean(vf * vf, axis=-1, keepdims=True) + 1e-6) * g).astype(jnp.bfloat16)


def pieces(v):
    out = []
    for _ in range(3):
        p = v.astype(jnp.bfloat16)
        out.append(p)
        v = v - p.astype(jnp.float32)
    return out


def dot(a, b, dims=((1,), (0,))):
    return lax.dot_general(a, b, (dims, ((), ())), preferred_element_type=jnp.float32)


def attention_body(nh, x_ref, ga_ref, gm_ref, wq_ref, wk_ref, wv_ref, wo_ref, h_ref, z_ref, u_ref, acc_ref):
    i = pl.program_id(0)

    @pl.when(i == 0)
    def _():
        u_ref[...] = rms(x_ref[...].astype(jnp.float32), ga_ref[...])
        acc_ref[...] = jnp.zeros_like(acc_ref)

    u = u_ref[...]
    seq = u.shape[0]
    half = seq // 2
    q = dot(u, wq_ref[...]).astype(jnp.bfloat16)
    k = dot(u, wk_ref[...]).astype(jnp.bfloat16)
    v = dot(u, wv_ref[...]).astype(jnp.bfloat16)
    tops, lows = [], []
    for j in range(nh):
        cols = slice(j * HEAD, (j + 1) * HEAD)
        for part, dst in ((0, tops), (1, lows)):
            n = half * (part + 1)
            s = dot(q[part * half:(part + 1) * half, cols], k[:n, cols], ((1,), (1,))) * HEAD ** -0.5
            row = lax.broadcasted_iota(jnp.int32, s.shape, 0) + part * half
            col = lax.broadcasted_iota(jnp.int32, s.shape, 1)
            s = jnp.where(row >= col, s, -1e30)
            e = jnp.exp(s - jnp.max(s, axis=-1, keepdims=True))
            p = (e * (1.0 / jnp.sum(e, axis=-1, keepdims=True))).astype(jnp.bfloat16)
            dst.append(dot(p, v[:n, cols]).astype(jnp.bfloat16))
    o = jnp.concatenate([jnp.concatenate(tops, axis=1), jnp.concatenate(lows, axis=1)], axis=0)
    acc_ref[...] += dot(o, wo_ref[...])

    @pl.when(i == pl.num_programs(0) - 1)
    def _():
        h = (x_ref[...].astype(jnp.float32) + acc_ref[...]).astype(jnp.bfloat16)
        h_ref[...] = h
        z_ref[...] = rms(h.astype(jnp.float32), gm_ref[...])


def attention(x, gattn, gmoe, wq, wk, wv, wo):
    seq, d = x.shape
    hd = wq.shape[1]
    nh = 2
    blk = nh * HEAD
    whole = lambda r: pl.BlockSpec((r, d), lambda i: (0, 0))
    wcol = pl.BlockSpec((d, blk), lambda i: (0, i))
    act = jax.ShapeDtypeStruct((seq, d), jnp.bfloat16)
    flops = 2 * seq * d * hd * 4 + 4 * seq * seq * hd
    return pl.pallas_call(
        functools.partial(attention_body, nh),
        grid=(hd // blk,),
        in_specs=[whole(seq), whole(1), whole(1), wcol, wcol, wcol, pl.BlockSpec((blk, d), lambda i: (i, 0))],
        out_specs=[whole(seq), whole(seq)],
        out_shape=[act, act],
        scratch_shapes=[pltpu.VMEM((seq, d), jnp.bfloat16), pltpu.VMEM((seq, d), jnp.float32)],
        compiler_params=pltpu.CompilerParams(vmem_limit_bytes=VMEM_LIMIT),
        cost_estimate=pl.CostEstimate(flops=flops, bytes_accessed=8 * d * hd, transcendentals=seq * seq * hd // HEAD),
        name="attn",
    )(x, gattn.reshape(1, d), gmoe.reshape(1, d), wq, wk, wv, wo)


def dispatch_body(slot_ref, z_ref, o_ref):
    slot = slot_ref[0]
    cores, slots, dh = o_ref.shape
    k = lax.broadcasted_iota(jnp.int32, (slots, slot.shape[1]), 0)
    r = dot((slot == k).astype(jnp.bfloat16), z_ref[...]).astype(jnp.bfloat16)
    for c in range(cores):
        o_ref[c] = r[:, c * dh:(c + 1) * dh]


def dispatch(slot, z):
    nc, _, t = slot.shape
    d = z.shape[1]
    return pl.pallas_call(
        dispatch_body,
        grid=(nc,),
        in_specs=[pl.BlockSpec((1, 1, t), lambda i: (i, 0, 0)), pl.BlockSpec((t, d), lambda i: (0, 0))],
        out_specs=pl.BlockSpec((CORES, SLOTS, d // CORES), lambda i: (i, 0, 0)),
        out_shape=jax.ShapeDtypeStruct((nc * CORES, SLOTS, d // CORES), jnp.bfloat16),
        compiler_params=pltpu.CompilerParams(vmem_limit_bytes=VMEM_LIMIT),
        cost_estimate=pl.CostEstimate(flops=2 * nc * SLOTS * t * d, bytes_accessed=2 * nc * SLOTS * d, transcendentals=0),
        name="dispatch",
    )(slot, z)


def experts_body(ns, cap, own_hbm, pos_ref, g_ref, w1_hbm, w3_hbm, w2_hbm, out_hbm,
                 w1_ref, w3_ref, w2_ref, x_ref, own_buf, oth_buf, sum_buf, snd_buf, in_buf,
                 w_sem, own_sem, rows_send, rows_recv, part_send, part_recv, out_sem, rows_free, part_free):
    i = pl.program_id(0)
    n = pl.num_programs(0)
    el, d, _ = w1_ref.shape
    dh = d // CORES
    slots = own_buf.shape[2]
    me = lax.axis_index("col")
    odd = lax.rem(me, CORES)
    peer = {"col": me + 1 - 2 * odd}
    mine = pl.ds(pl.multiple_of(odd * dh, dh), dh)
    his = pl.ds(pl.multiple_of((1 - odd) * dh, dh), dh)

    def loads(e):
        out = []
        for j, (src, dst) in enumerate(((w1_hbm, w1_ref), (w3_hbm, w3_ref))):
            out.append(pltpu.make_async_copy(src.at[e, mine], dst.at[e, 0:dh], w_sem.at[2 * j, e]))
            out.append(pltpu.make_async_copy(src.at[e, his], dst.at[e, dh:d], w_sem.at[2 * j + 1, e]))
        out.append(pltpu.make_async_copy(w2_hbm.at[e, :, mine], w2_ref.at[e, :, 0:dh], w_sem.at[4, e]))
        out.append(pltpu.make_async_copy(w2_hbm.at[e, :, his], w2_ref.at[e, :, dh:d], w_sem.at[5, e]))
        return out

    def local_rows(j):
        b = lax.rem(j, 2)
        return pltpu.make_async_copy(own_hbm.at[pl.ds(j * ns, ns)], own_buf.at[b], own_sem.at[b])

    def peer_rows(j):
        b = lax.rem(j, 2)
        return pltpu.make_async_remote_copy(
            src_ref=own_hbm.at[pl.ds(j * ns, ns)], dst_ref=oth_buf.at[b], send_sem=rows_send.at[b],
            recv_sem=rows_recv.at[b], device_id=peer, device_id_type=pl.DeviceIdType.MESH)

    def peer_part(j):
        b = lax.rem(j, 2)
        return pltpu.make_async_remote_copy(
            src_ref=snd_buf.at[b], dst_ref=in_buf.at[b], send_sem=part_send.at[b],
            recv_sem=part_recv.at[b], device_id=peer, device_id_type=pl.DeviceIdType.MESH)

    def result(j):
        b = lax.rem(j, 2)
        return pltpu.make_async_copy(sum_buf.at[b], out_hbm.at[pl.ds(j * ns, ns)], out_sem.at[b])

    def tell(sem):
        pl.semaphore_signal(sem, inc=1, device_id=peer, device_id_type=pl.DeviceIdType.MESH)

    b = lax.rem(i, 2)
    o = 1 - b

    @pl.when(i == 0)
    def _():
        for e in range(el):
            for c in loads(e):
                c.start()
        local_rows(i).start()
        barrier = pltpu.get_barrier_semaphore()
        tell(barrier)
        pl.semaphore_wait(barrier, 1)
        peer_rows(i).start()

    @pl.when(i + 1 < n)
    def _():
        local_rows(i + 1).start()

        @pl.when(i >= 1)
        def _():
            pl.semaphore_wait(rows_free, 1)

        peer_rows(i + 1).start()

    local_rows(i).wait()
    peer_rows(i).wait()

    rank = lax.broadcasted_iota(jnp.int32, (el, cap, slots), 1)
    for s in range(ns):
        hit = (pos_ref[s][:, None, :] == rank).astype(jnp.bfloat16).reshape(el * cap, slots)
        for k, buf in ((0, own_buf), (1, oth_buf)):
            xs = dot(hit, buf[b, s]).astype(jnp.bfloat16)
            for e in range(el):
                x_ref[e, s * cap:(s + 1) * cap, k * dh:(k + 1) * dh] = xs[e * cap:(e + 1) * cap]

    @pl.when(i + 2 < n)
    def _():
        tell(rows_free)

    def expert(e, _):
        @pl.when(i == 0)
        def _():
            for c in loads(e):
                c.wait()

        x = x_ref[e]
        h1 = dot(x, w1_ref[e])
        h3 = dot(x, w3_ref[e])
        a = (jax.nn.silu(h1) * h3).astype(jnp.bfloat16)
        x_ref[e] = dot(a, w2_ref[e]).astype(jnp.bfloat16)
        return 0

    lax.fori_loop(0, el, expert, 0)

    def finish(j, b):
        peer_part(j).wait()
        sum_buf[b] += in_buf[b]

        @pl.when(j + 2 < n)
        def _():
            tell(part_free)

        result(j).start()

    @pl.when(i >= 2)
    def _():
        result(i - 2).wait()

    for s in range(ns):
        w = jnp.where(pos_ref[s][:, None, :] == rank, g_ref[s][:, None, :], 0.0).reshape(el * cap, slots)
        w = jnp.concatenate(pieces(w), axis=1)
        for k, buf in ((0, sum_buf), (1, snd_buf)):
            out = jnp.concatenate([x_ref[e, s * cap:(s + 1) * cap, k * dh:(k + 1) * dh] for e in range(el)], axis=0)
            p3 = dot(w, out, ((0,), (0,)))
            buf[b, s] = p3[:slots] + p3[slots:2 * slots] + p3[2 * slots:]

    @pl.when(i >= 1)
    def _():
        finish(i - 1, o)

    @pl.when(i >= 2)
    def _():
        pl.semaphore_wait(part_free, 1)

    peer_part(i).start()

    @pl.when(i == n - 1)
    def _():
        finish(i, b)
        result(i - 1).wait()
        result(i).wait()


def experts(own, pos, g, w1, w3, w2, cap, call):
    n, slots, dh = own.shape
    el, d, f = w1.shape
    ns = 4
    meta = pl.BlockSpec((ns, el, slots), lambda i: (i, 0, 0))
    hbm = pl.BlockSpec(memory_space=pl.ANY)
    flops = 6 * n * el * cap * d * f
    block = (2, ns, slots, dh)
    two = pltpu.SemaphoreType.DMA((2,))
    return pl.pallas_call(
        functools.partial(experts_body, ns, cap),
        grid=(n // ns,),
        in_specs=[hbm, meta, meta, hbm, hbm, hbm],
        out_specs=hbm,
        out_shape=jax.ShapeDtypeStruct((n, slots, dh), jnp.float32),
        scratch_shapes=[
            pltpu.VMEM((el, d, f), jnp.bfloat16),
            pltpu.VMEM((el, d, f), jnp.bfloat16),
            pltpu.VMEM((el, f, d), jnp.bfloat16),
            pltpu.VMEM((el, ns * cap, d), jnp.bfloat16),
            pltpu.VMEM(block, jnp.bfloat16),
            pltpu.VMEM(block, jnp.bfloat16),
            pltpu.VMEM(block, jnp.float32),
            pltpu.VMEM(block, jnp.float32),
            pltpu.VMEM(block, jnp.float32),
            pltpu.SemaphoreType.DMA((6, el)),
            two, two, two, two, two, two,
            pltpu.SemaphoreType.REGULAR,
            pltpu.SemaphoreType.REGULAR,
        ],
        compiler_params=pltpu.CompilerParams(vmem_limit_bytes=VMEM_LIMIT, collective_id=call, has_side_effects=True),
        cost_estimate=pl.CostEstimate(flops=flops, bytes_accessed=6 * el * d * f + 12 * n * slots * dh, transcendentals=n * el * cap * f),
        name="experts",
    )(own, pos, g, w1, w3, w2)


def combine_body(slot_ref, ret_ref, h_ref, acc_in_ref, y_ref, acc_ref):
    i = pl.program_id(0)

    @pl.when(i == 0)
    def _():
        acc_ref[...] = acc_in_ref[...] if acc_in_ref is not None else jnp.zeros_like(acc_ref)

    nc, _, t = slot_ref.shape
    _, slots, dh = ret_ref.shape
    k = lax.broadcasted_iota(jnp.int32, (slots, t), 0)
    sel = [(slot_ref[c] == k).astype(jnp.bfloat16) for c in range(nc)]
    for j in range(CORES):
        cols = slice(j * dh, (j + 1) * dh)
        for c in range(nc):
            for p in pieces(ret_ref[c * CORES + j]):
                acc_ref[:, cols] += dot(sel[c], p, ((0,), (0,)))

    @pl.when(i == pl.num_programs(0) - 1)
    def _():
        y_ref[...] = (h_ref[...].astype(jnp.float32) + acc_ref[...]).astype(jnp.bfloat16)


def combine(slot, ret, h, acc=None):
    nc, _, t = slot.shape
    d = h.shape[1]
    nb = 2
    whole = pl.BlockSpec((t, d), lambda i: (0, 0))
    specs = [pl.BlockSpec((nb, 1, t), lambda i: (i, 0, 0)),
             pl.BlockSpec((nb * CORES, SLOTS, d // CORES), lambda i: (i, 0, 0)), whole]
    args = [slot, ret, h]
    body = combine_body
    if acc is None:
        body = lambda s, r, h, y, a: combine_body(s, r, h, None, y, a)
    else:
        specs.append(whole)
        args.append(acc)
    return pl.pallas_call(
        body,
        grid=(nc // nb,),
        in_specs=specs,
        out_specs=[whole, whole],
        out_shape=[jax.ShapeDtypeStruct((t, d), jnp.bfloat16), jax.ShapeDtypeStruct((t, d), jnp.float32)],
        compiler_params=pltpu.CompilerParams(vmem_limit_bytes=VMEM_LIMIT),
        cost_estimate=pl.CostEstimate(flops=6 * nc * SLOTS * t * d, bytes_accessed=4 * nc * SLOTS * d, transcendentals=0),
        name="combine",
    )(*args)


def experts_plain(own, oth, odd, pos, g, w1, w3, w2, cap):
    rows = jnp.concatenate([jnp.where(odd, oth, own), jnp.where(odd, own, oth)], axis=-1)

    def one(total, e):
        pos, g, a1, a3, a2 = e
        hit = pos[:, None, :] == jnp.arange(cap, dtype=jnp.int32)[None, :, None]
        x = jnp.einsum("sck,skd->scd", hit.astype(jnp.bfloat16), rows, preferred_element_type=jnp.float32).astype(jnp.bfloat16)
        h1 = jnp.einsum("scd,df->scf", x, a1, preferred_element_type=jnp.float32)
        h3 = jnp.einsum("scd,df->scf", x, a3, preferred_element_type=jnp.float32)
        a = (jax.nn.silu(h1) * h3).astype(jnp.bfloat16)
        o = jnp.einsum("scf,fd->scd", a, a2, preferred_element_type=jnp.float32).astype(jnp.bfloat16)
        for w in pieces(jnp.where(hit, g[:, None, :], 0.0)):
            total = total + jnp.einsum("sck,scd->skd", w, o, preferred_element_type=jnp.float32)
        return total, None

    total, _ = lax.scan(one, jnp.zeros(rows.shape, jnp.float32), (pos.swapaxes(0, 1), g.swapaxes(0, 1), w1, w3, w2))
    left, right = jnp.split(total, CORES, axis=-1)
    return jnp.where(odd, right, left), jnp.where(odd, left, right)


def chip_ranks(idx, nc, epc):
    t = idx.shape[0]
    hit = jnp.any((idx // epc)[:, :, None] == jnp.arange(nc, dtype=idx.dtype), axis=1)
    tri = (jnp.arange(t)[:, None] > jnp.arange(t)[None, :]).astype(jnp.bfloat16)
    rank = dot(tri, hit.astype(jnp.bfloat16)).astype(jnp.int32)
    return jnp.where(hit, rank, -1).T.reshape(nc, 1, t), jnp.max(jnp.sum(hit, axis=0))


def slot_gates(slot, gm):
    nc, _, t = slot.shape
    sel = (slot == jnp.arange(SLOTS, dtype=jnp.int32)[None, :, None]).astype(jnp.bfloat16)
    g = jnp.stack(pieces(gm.reshape(t, nc, -1)))
    out = jnp.einsum("ckt,ptce->pcek", sel, g, preferred_element_type=jnp.float32)
    return out[0] + (out[1] + out[2])


def solution(mesh):
    ep_axes = ("row", "col")
    tok_axes = ("dp", "row", "col")
    ncol = mesh.shape["col"]
    ep = mesh.shape["row"] * ncol
    nc = ep // CORES
    pair = [(i, i ^ 1) for i in range(ncol)]

    def local(x, idx, gates, wq, wk, wv, wo, gattn, gmoe, w1, w3, w2):
        nm, ns, seq, d = x.shape
        t = ns * seq
        top = idx.shape[-1]
        el = w1.shape[0]
        n_exp = el * ep
        cap = capacity(t, top, n_exp)
        odd = lax.axis_index("col") % CORES == 1

        ranks, most, dense = [], [], []
        for m in range(nm):
            im = idx[m].reshape(t, top)
            rank, count = chip_ranks(im, nc, n_exp // nc)
            ranks.append(rank)
            most.append(count)
            hit = im[:, :, None] == jnp.arange(n_exp, dtype=im.dtype)
            dense.append(jnp.sum(jnp.where(hit, gates[m].reshape(t, top)[:, :, None], 0.0), axis=1))

        def exchange_gates(r):
            g = [slot_gates(ranks[m] - r * SLOTS, dense[m]).reshape(ep, el, SLOTS) for m in range(nm)]
            top_count = functools.reduce(jnp.maximum, most).astype(jnp.float32)
            g.append(jnp.broadcast_to(top_count, (ep, 8, SLOTS)))
            got = lax.all_to_all(jnp.concatenate(g, axis=1), ep_axes, 0, 0, tiled=True)
            out = []
            for m in range(nm):
                gm = got[:, m * el:(m + 1) * el]
                hit = gm > 0.0
                tri = (jnp.arange(SLOTS)[:, None] < jnp.arange(SLOTS)[None, :]).astype(jnp.bfloat16)
                pos = dot(hit.astype(jnp.bfloat16).reshape(ep * el, SLOTS), tri).astype(jnp.int32).reshape(hit.shape)
                out.append((jnp.where(hit, pos, -1), gm))
            return out, jnp.max(got[:, nm * el:])

        def send(m, r, z):
            return lax.all_to_all(dispatch(ranks[m] - r * SLOTS, z), ep_axes, 0, 0, tiled=True)

        def give_back(own, meta, call):
            total = experts(own, meta[0], meta[1], w1, w3, w2, cap, call)
            return lax.all_to_all(total, ep_axes, 0, 0, tiled=True)

        meta, most_all = exchange_gates(0)
        hs, zs = [], []
        recv = []
        for m in range(nm):
            h, z = attention(x[m].reshape(t, d), gattn, gmoe, wq, wk, wv, wo)
            if m == 0:
                z, meta, most_all = lax.optimization_barrier((z, meta, most_all))
            hs.append(h)
            zs.append(z)
            recv.append(send(m, 0, z))
        ys, accs = [], []
        for m in range(nm):
            ret = give_back(recv[m], meta[m], m)
            y, acc = combine(ranks[m], ret, hs[m])
            ys.append(y)
            accs.append(acc)

        rounds = (most_all.astype(jnp.int32) + SLOTS - 1) // SLOTS

        def more(ys):
            z, h, slot = jnp.stack(zs), jnp.stack(hs), jnp.stack(ranks)

            def body(c):
                j, ys, accs = c
                r, m = j // nm, j % nm
                meta, _ = exchange_gates(r)
                pos, g = (jnp.where(m == 0, meta[0][k], meta[1][k]) for k in range(2))
                s = slot[m] - r * SLOTS
                own = lax.all_to_all(dispatch(s, z[m]), ep_axes, 0, 0, tiled=True)
                mine, his = experts_plain(own, lax.ppermute(own, "col", pair), odd, pos, g, w1, w3, w2, cap)
                ret = lax.all_to_all(mine + lax.ppermute(his, "col", pair), ep_axes, 0, 0, tiled=True)
                y, acc = combine(s, ret, h[m], accs[m])
                return j + 1, ys.at[m].set(y), accs.at[m].set(acc)

            _, ys, _ = lax.while_loop(lambda c: c[0] < rounds * nm, body, (jnp.int32(nm), jnp.stack(ys), jnp.stack(accs)))
            return tuple(ys[m] for m in range(nm))

        ys = lax.cond(rounds > 1, more, lambda ys: ys, tuple(ys))
        return jnp.stack([y.reshape(ns, seq, d) for y in ys])

    tok_spec = P(None, tok_axes)
    exp_spec = P(ep_axes)
    return jax.shard_map(local, mesh=mesh,
                         in_specs=(tok_spec, tok_spec, tok_spec, P(), P(), P(), P(), P(), P(), exp_spec, exp_spec, exp_spec),
                         out_specs=tok_spec, check_vma=False)
```
